256 devices in a mesh: grp: 2 (over z), row: 64 (over y, x), col: 2 (over core).
Axes of the slice: x: 8, y: 8, z: 2, core: 2. Of those that a mesh axis runs over, the one named last changes fastest.
The devices are a block of a 8x8x16 slice.
Arguments:
- factors: bfloat16 [2, 12288, 6144], P(None, ('grp', 'row'), 'col'), parts along dimension 1, may hold values from -6 to 6
- orbitals: bfloat16 [12288, 1024], P(('grp', 'row'), 'col'), parts along dimension 0, may hold values from -0.02734375 to 0.02734375
- field_term: bfloat16 [12288, 6144], P(('grp', 'row'), 'col'), parts along dimension 0, may hold values from -1.5 to 1.5
Outputs:
- fock_matrix: bfloat16 [12288, 6144], P(('grp', 'row'), 'col'), parts along dimension 0
The draws below stay inside these ranges and needn't reach their ends.
There are 2 independent parts, one for each index of `grp`. The reference program is written for one: setup_inputs(seed, part) draws one part's arguments, and reference() takes and returns one part's arrays. A program takes and returns all parts, laid end to end along the dimension named above; each array names one. Nothing has to cross between parts.
All inputs are finite; a program needn't handle non-finite values.
Results may differ from the reference program's by a relative error of at most 0.02.
Values may be sent and summed in bfloat16 or wider, within the bound.
No kernel may reach another device: no remote copies, remote signals or barrier semaphores. Data moves between devices by JAX's collectives and lax.ppermute only.
A program may use at most 64 MiB of HBM per device.

```python
import jax
import jax.numpy as jnp

N = 6144
NOCC = 1024
NAUX = 2


def steps_of(rng, extent, pieces, smallest, top_value):
    gain, own = 1.0, jax.random.fold_in(rng, 6)
    for axis_at, shards_of in pieces:
        draws = jnp.exp(jax.random.uniform(jax.random.fold_in(own, axis_at), (shards_of,), jnp.float32, smallest / len(pieces), top_value / len(pieces)))
        gain = gain * jnp.repeat(draws, extent[axis_at] // shards_of).reshape([-1 if axis == axis_at else 1 for axis in range(len(extent))])
    return gain


def normal_values(stream_key, shape, width, limit, shards=(), kind=jnp.bfloat16):
    loudness = steps_of(stream_key, shape, shards, -0.22, 0.18) if shards else 1.0
    array = jax.random.normal(stream_key, shape, jnp.float32) * width * loudness
    return jnp.minimum(jnp.maximum(array, -limit), limit).astype(kind)


def setup_inputs(seed: int = 0, part: int = 0) -> dict:
    streams_of = jax.random.split(jax.random.key(seed), 4)
    part_splits = jax.random.split(jax.random.fold_in(streams_of[3], part), 4)
    return {
        "factors": normal_values(part_splits[0], (NAUX, N, N), 1.0, 6.0, ((1, 64), (2, 2))),
        "orbitals": normal_values(part_splits[1], (N, NOCC), (N * 8) ** -0.5, 0.02734375, ((0, 64), (1, 2))),
        "field_term": normal_values(part_splits[2], (N, N), 0.25, 1.5, ((0, 64), (1, 2))),
    }


def reference(factors, orbitals, field_term):
    orbit_wide = orbitals.astype(jnp.float32)
    exchange = jnp.zeros((N, N), jnp.float32)
    coulomb = jnp.zeros((N, N), jnp.float32)
    for aux in range(NAUX):
        half_aux = jnp.dot(factors[aux], orbitals, preferred_element_type=jnp.float32).astype(jnp.bfloat16)
        gamma_aux = jnp.sum(half_aux.astype(jnp.float32) * orbit_wide)
        exchange = exchange + jnp.dot(half_aux, half_aux.T, preferred_element_type=jnp.float32)
        coulomb = coulomb + gamma_aux * factors[aux].astype(jnp.float32)
    fock_matrix = field_term.astype(jnp.float32) + coulomb - 0.25 * exchange
    return fock_matrix.astype(jnp.bfloat16)
```

```python
import math

import jax
import jax.numpy as jnp
from jax import lax
from jax.sharding import Mesh
from jax.sharding import PartitionSpec as P

GRP_ROW = ("grp", "row_0", "row_1")
Y, X = "row_0", "row_1"


def partner(i, n, parity):
    return i ^ 1 if parity == 0 else (((i + 1) ^ 1) - 1) % n


def swap(value, axis, parity):
    n = lax.axis_size(axis)
    return lax.ppermute(value, axis, [(i, partner(i, n, parity)) for i in range(n)])


def other_core(value):
    return lax.ppermute(value, "col", [(0, 1), (1, 0)])


def ring_gather(own, axis, parity, place, into):
    n = lax.axis_size(axis)
    me = lax.axis_index(axis)
    sign = jnp.where((me + parity) % 2 == 0, 1, -1)

    def at(offset):
        return (me + sign * offset + n) % n

    into = place(into, own, me)
    held = swap(own, axis, parity)
    into = place(into, held, at(1))
    sent = jnp.stack([own, held])
    side = -1
    reach = 1
    for step in range(1, n // 2):
        sent = swap(sent, axis, (parity + step) % 2)
        for k in range(2):
            into = place(into, sent[k], at(side * (reach + k)))
        side = -side
        reach += 1
    return into


def put_major(buffer, piece, index):
    return lax.dynamic_update_index_in_dim(buffer, piece, index, 0)


def put_second(buffer, piece, index):
    return lax.dynamic_update_index_in_dim(buffer, piece, index, 1)


def gather_orbitals(part, first, parity):
    ny, nx = lax.axis_size(Y), lax.axis_size(X)
    rows, columns = part.shape
    whole = jnp.zeros((ny, nx, rows, columns), part.dtype)
    if first == X:
        line = ring_gather(part, X, parity, put_major, jnp.zeros((nx, rows, columns), part.dtype))
        return ring_gather(line, Y, parity, put_major, whole)
    line = ring_gather(part, Y, parity, put_major, jnp.zeros((ny, rows, columns), part.dtype))
    return ring_gather(line, X, parity, put_second, whole)


def butterfly_sum(value):
    for axis in (X, Y, "col"):
        n = lax.axis_size(axis)
        bit = 1
        while bit < n:
            value = value + lax.ppermute(value, axis, [(i, i ^ bit) for i in range(n)])
            bit *= 2
    return value


def shards(factors, orbitals, field_term):
    aux_count, rows, half_n = factors.shape
    ny, nx = lax.axis_size(Y), lax.axis_size(X)
    core = lax.axis_index("col")
    factors_other = other_core(factors)

    quarter = orbitals.shape[1] // 4
    streams = ((X, 0), (Y, 0), (X, 1), (Y, 1))
    gathered = [
        gather_orbitals(orbitals[:, q * quarter : (q + 1) * quarter], *stream)
        for q, stream in enumerate(streams)
    ]
    all_orbitals = jnp.concatenate([g.reshape(2, half_n, quarter) for g in gathered], axis=2)
    orbitals_mine = lax.dynamic_index_in_dim(all_orbitals, core, 0, False)
    orbitals_other = lax.dynamic_index_in_dim(all_orbitals, 1 - core, 0, False)

    orbit_wide = orbitals.astype(jnp.float32)
    block = jnp.zeros((ny * rows, nx * rows), jnp.float32)
    fits = []
    for aux in range(aux_count):
        half_local = (
            jnp.dot(factors[aux], orbitals_mine, preferred_element_type=jnp.float32)
            + jnp.dot(factors_other[aux], orbitals_other, preferred_element_type=jnp.float32)
        ).astype(jnp.bfloat16)
        fits.append(jnp.sum(half_local.astype(jnp.float32) * orbit_wide))
        empty = jnp.zeros((nx, *half_local.shape), half_local.dtype)
        along_x = ring_gather(half_local, X, aux % 2, put_major, empty)
        along_y = ring_gather(half_local, Y, aux % 2, put_major, empty)
        block = block + lax.dot_general(
            along_y.reshape(ny * rows, -1),
            along_x.reshape(nx * rows, -1),
            (((1,), (1,)), ((), ())),
            preferred_element_type=jnp.float32,
        )
    fitted = butterfly_sum(jnp.broadcast_to(jnp.stack(fits)[:, None], (aux_count, 128)))

    width = nx * rows // 2
    mine = lax.dynamic_slice_in_dim(block, core * width, width, 1)
    theirs = lax.dynamic_slice_in_dim(block, (1 - core) * width, width, 1)
    arrived = other_core(theirs.astype(jnp.bfloat16))
    total = (mine + arrived.astype(jnp.float32)).astype(jnp.bfloat16)
    returned = lax.all_to_all(total.reshape(ny, rows, width), Y, 0, 0, tiled=True)
    returned = returned.reshape(2, ny // 2, rows, width)
    kept = lax.dynamic_index_in_dim(returned, core, 0, False)
    swapped = other_core(lax.dynamic_index_in_dim(returned, 1 - core, 0, False))
    first = jnp.where(core == 0, kept, swapped)
    second = jnp.where(core == 0, swapped, kept)
    exchange = jnp.concatenate([first, second], axis=2)
    exchange = jnp.concatenate(list(exchange), axis=1)

    coulomb = jnp.zeros(field_term.shape, jnp.float32)
    for aux in range(aux_count):
        coulomb = coulomb + fitted[aux, 0] * factors[aux].astype(jnp.float32)
    fock_matrix = (
        field_term.astype(jnp.float32) + coulomb - 0.25 * exchange.astype(jnp.float32)
    )
    return fock_matrix.astype(jnp.bfloat16)


def solution(mesh):
    side = math.isqrt(mesh.shape["row"])
    finer = Mesh(
        mesh.devices.reshape(mesh.shape["grp"], side, side, mesh.shape["col"]),
        ("grp", Y, X, "col"),
    )
    return jax.shard_map(
        shards,
        mesh=finer,
        in_specs=(P(None, GRP_ROW, "col"), P(GRP_ROW, "col"), P(GRP_ROW, "col")),
        out_specs=P(GRP_ROW, "col"),
        check_vma=False,
    )
```

```python
import functools
import math

import jax
import jax.numpy as jnp
from jax import lax
from jax.experimental import pallas as pl
from jax.experimental.pallas import tpu as pltpu
from jax.sharding import Mesh
from jax.sharding import PartitionSpec as P

GRP_ROW = ("grp", "row_0", "row_1")
Y, X = "row_0", "row_1"
TILE = 8


def partner(i, n, parity):
    return i ^ 1 if parity == 0 else (((i + 1) ^ 1) - 1) % n


def swap(value, axis, parity):
    n = lax.axis_size(axis)
    return lax.ppermute(value, axis, [(i, partner(i, n, parity)) for i in range(n)])


def swap_by_core(value, parity, phase):
    ny, nx = lax.axis_size(Y), lax.axis_size(X)
    pairs = []
    for y in range(ny):
        for x in range(nx):
            for core in range(2):
                to_y, to_x = y, x
                if core == phase:
                    to_x = partner(x, nx, parity)
                else:
                    to_y = partner(y, ny, parity)
                pairs.append(((y * nx + x) * 2 + core, (to_y * nx + to_x) * 2 + core))
    return lax.ppermute(value, (Y, X, "col"), pairs)


def other_core(value):
    return lax.ppermute(value, "col", [(0, 1), (1, 0)])


def source(slot, me, parity, n):
    sign = 1 - 2 * lax.rem(me + parity, 2)
    pair = lax.div(slot, 2)
    side = 1 - 2 * lax.rem(pair, 2)
    offset = jnp.where(slot < 2, slot, side * (pair + lax.rem(slot, 2)))
    return lax.rem(me + sign * offset + n, n)


def ring_steps(own, exchange, n):
    held = exchange(own, 0)
    yield held[None]
    sent = jnp.stack([own, held])
    for step in range(1, n // 2):
        sent = exchange(sent, step)
        yield sent


def accumulate_kernel(parity, first_slot, factor_ref, piece_ref, *rest):
    (sum_ref,) = rest[-1:]
    y, x, core = lax.axis_index(Y), lax.axis_index(X), lax.axis_index("col")
    ny, nx = lax.axis_size(Y), lax.axis_size(X)
    n = nx
    major = jnp.where(core == 0, y, x)
    minor = jnp.where(core == 0, x, y)
    pieces, line = piece_ref.shape[:2]
    total = ny * nx

    def add(step, acc):
        far = source(first_slot + lax.div(step, line), major, parity, n)
        near = source(lax.rem(step, line), minor, parity, n)
        block = jnp.where(core == 0, far * nx + near, near * nx + far)
        at = lax.rem(block - core * (total // 2) + total, total)
        return acc + jnp.dot(
            factor_ref[at],
            piece_ref[lax.div(step, line), lax.rem(step, line)],
            preferred_element_type=jnp.float32,
        )

    before = jnp.zeros(sum_ref.shape, jnp.float32) if len(rest) == 1 else rest[0][...]
    sum_ref[...] = lax.fori_loop(0, pieces * line, add, before, unroll=2)


def accumulate(factor_blocks, piece, before, parity, first_slot):
    pieces, line, rows, columns = piece.shape
    out = jax.ShapeDtypeStruct((factor_blocks.shape[1], columns), jnp.float32)
    given = (factor_blocks, piece) if before is None else (factor_blocks, piece, before)
    vmem = pl.BlockSpec(memory_space=pltpu.VMEM)
    return pl.pallas_call(
        functools.partial(accumulate_kernel, parity, first_slot),
        out_shape=out,
        in_specs=[vmem] * len(given),
        out_specs=vmem,
        input_output_aliases={} if before is None else {2: 0},
        cost_estimate=pl.CostEstimate(
            flops=2 * pieces * line * rows * columns * out.shape[0],
            bytes_accessed=piece.size * 2,
            transcendentals=0,
        ),
    )(*given)


def half_transform(factor_blocks, part, parity):
    n = lax.axis_size(X)
    phase = lambda which: lambda value, step: swap_by_core(value, (parity + step) % 2, which)
    line = jnp.concatenate([part[None], *ring_steps(part, phase(0), n)])
    total = accumulate(factor_blocks, line[None], None, parity, 0)
    slot = 1
    for arrived in ring_steps(line, phase(1), n):
        total = accumulate(factor_blocks, arrived, total, parity, slot)
        slot += arrived.shape[0]
    return total


def put(into, piece, index):
    return lax.dynamic_update_index_in_dim(into, piece, index, 0)


def gather_rows(own, axis, parity, rows):
    n, me = lax.axis_size(axis), lax.axis_index(axis)
    into = jnp.zeros((n, rows, own.shape[1]), own.dtype)
    into = put(into, own[:rows], me)
    under = [own[rows:]]
    slot = 1
    for arrived in ring_steps(own, lambda v, step: swap(v, axis, (parity + step) % 2), n):
        for piece in arrived:
            into = put(into, piece[:rows], source(slot, me, parity, n))
            under.append(piece[rows:])
            slot += 1
    return into, under


def in_parts(value):
    parts = []
    for _ in range(3):
        part = lax.reduce_precision(value, 8, 7)
        parts.append(part)
        value = value - part
    return jnp.stack(parts, axis=-1).astype(jnp.bfloat16)


def tile_of(values, columns):
    flat = in_parts(values).reshape(-1)
    return jnp.pad(flat[None], ((0, TILE - 1), (0, columns - flat.size)))


def shards(factors, orbitals, field_term):
    aux_count, rows, half_n = factors.shape
    ny, nx = lax.axis_size(Y), lax.axis_size(X)
    core = lax.axis_index("col")

    def blocks(part):
        return part.reshape(aux_count * rows, -1, rows).transpose(1, 0, 2)

    factor_blocks = jnp.concatenate([blocks(factors), blocks(other_core(factors))])
    width = orbitals.shape[1] // 2
    halves = [
        half_transform(factor_blocks, orbitals[:, q * width : (q + 1) * width], q)
        for q in range(2)
    ]
    half = jnp.concatenate(halves, axis=1).astype(jnp.bfloat16)
    half = half.reshape(aux_count, rows, -1)

    orbit_wide = orbitals.astype(jnp.float32)
    fits = []
    gathered = []
    for aux in range(aux_count):
        fit = jnp.sum(half[aux].astype(jnp.float32) * orbit_wide)
        with_fit = jnp.concatenate([half[aux], tile_of(fit[None], half.shape[2])])
        along_y, _ = gather_rows(half[aux], Y, aux % 2, rows)
        along_x, under = gather_rows(with_fit, X, aux % 2, rows)
        fits.append(sum(u[0, :3].astype(jnp.float32) for u in under).sum())
        gathered.append((along_y.reshape(ny * rows, -1), along_x))

    def block_half(which):
        total = None
        for along_y, along_x in gathered:
            columns = lax.dynamic_slice_in_dim(along_x, which * (nx // 2), nx // 2, 0)
            term = lax.dot_general(
                along_y,
                columns.reshape(nx // 2 * rows, -1),
                (((1,), (1,)), ((), ())),
                preferred_element_type=jnp.float32,
            )
            total = term if total is None else total + term
        return total

    width = nx // 2 * rows
    fit = jnp.stack(fits)
    theirs = jnp.concatenate(
        [block_half(1 - core).astype(jnp.bfloat16), tile_of(fit, width)]
    )
    arrived = other_core(theirs)
    total = block_half(core) + arrived[:-TILE].astype(jnp.float32)
    count = 3 * aux_count
    fit = fit + arrived[-TILE, :count].astype(jnp.float32).reshape(aux_count, 3).sum(1)
    tiles = jnp.broadcast_to(tile_of(fit, width), (ny, TILE, width))
    total = total.astype(jnp.bfloat16).reshape(ny, rows, width)
    returned = lax.all_to_all(
        jnp.concatenate([total, tiles], axis=1), Y, 0, 0, tiled=True
    )
    fitted = returned[:, rows, :count].astype(jnp.float32).reshape(ny, aux_count, 3).sum((0, 2))
    returned = returned[:, :rows].reshape(2, ny // 2, rows, width)
    kept = lax.dynamic_index_in_dim(returned, core, 0, False)
    swapped = other_core(lax.dynamic_index_in_dim(returned, 1 - core, 0, False))
    first = jnp.where(core == 0, kept, swapped)
    second = jnp.where(core == 0, swapped, kept)
    exchange = jnp.concatenate([first, second], axis=2)
    exchange = jnp.concatenate(list(exchange), axis=1)

    coulomb = jnp.zeros(field_term.shape, jnp.float32)
    for aux in range(aux_count):
        coulomb = coulomb + fitted[aux] * factors[aux].astype(jnp.float32)
    fock_matrix = (
        field_term.astype(jnp.float32) + coulomb - 0.25 * exchange.astype(jnp.float32)
    )
    return fock_matrix.astype(jnp.bfloat16)


def solution(mesh):
    side = math.isqrt(mesh.shape["row"])
    finer = Mesh(
        mesh.devices.reshape(mesh.shape["grp"], side, side, mesh.shape["col"]),
        ("grp", Y, X, "col"),
    )
    return jax.shard_map(
        shards,
        mesh=finer,
        in_specs=(P(None, GRP_ROW, "col"), P(GRP_ROW, "col"), P(GRP_ROW, "col")),
        out_specs=P(GRP_ROW, "col"),
        check_vma=False,
    )
```

```python
import functools
import math

import jax
import jax.numpy as jnp
from jax import lax
from jax.experimental import pallas as pl
from jax.experimental.pallas import tpu as pltpu
from jax.sharding import Mesh
from jax.sharding import PartitionSpec as P

GRP_ROW = ("grp", "row_0", "row_1")
Y, X = "row_0", "row_1"
TILE = 8


def partner(i, n, parity):
    return i ^ 1 if parity == 0 else (((i + 1) ^ 1) - 1) % n


def swap(value, axis, parity):
    n = lax.axis_size(axis)
    return lax.ppermute(value, axis, [(i, partner(i, n, parity)) for i in range(n)])


def swap_by_core(value, parity, phase):
    ny, nx = lax.axis_size(Y), lax.axis_size(X)
    pairs = []
    for y in range(ny):
        for x in range(nx):
            for core in range(2):
                to_y, to_x = y, x
                if core == phase:
                    to_x = partner(x, nx, parity)
                else:
                    to_y = partner(y, ny, parity)
                pairs.append(((y * nx + x) * 2 + core, (to_y * nx + to_x) * 2 + core))
    return lax.ppermute(value, (Y, X, "col"), pairs)


def other_core(value):
    return lax.ppermute(value, "col", [(0, 1), (1, 0)])


def source(slot, me, parity, n):
    sign = 1 - 2 * lax.rem(me + parity, 2)
    pair = lax.div(slot, 2)
    side = 1 - 2 * lax.rem(pair, 2)
    offset = jnp.where(slot < 2, slot, side * (pair + lax.rem(slot, 2)))
    return lax.rem(me + sign * offset + n, n)


def ring_steps(own, exchange, n):
    held = exchange(own, 0)
    yield held[None]
    sent = jnp.stack([own, held])
    for step in range(1, n // 2):
        sent = exchange(sent, step)
        yield sent


def piece_streams(part, parity):
    n = lax.axis_size(X)

    def phase(which):
        return lambda value, step: swap_by_core(value, (parity + step) % 2, which)

    steps = list(ring_steps(part, phase(0), n))
    lines = (
        jnp.concatenate([part[None], *steps[: n // 4]]),
        jnp.concatenate(steps[n // 4 :]),
    )
    return [(line[None], *ring_steps(line, phase(1), n)) for line in lines]


def half_kernel(shape, mine_ref, other_ref, *refs):
    half_ref, line_ref, ordered_ref, sum_ref = refs[-4:]
    arrivals = list(refs[:-4])
    y, x, core = lax.axis_index(Y), lax.axis_index(X), lax.axis_index("col")
    ny, nx = shape
    n, count = nx, ny * nx
    major, minor = jnp.where(core == 0, y, x), jnp.where(core == 0, x, y)
    columns = arrivals[0].shape[-1]
    for parity in range(2):
        for first_near in (0, n // 2):
            slot = 0
            while slot < n:
                ref = arrivals.pop(0)
                for p in range(ref.shape[0]):
                    far = source(slot, major, parity, n)
                    slot += 1
                    for i in range(n // 2):
                        near = source(first_near + i, minor, parity, n)
                        block = jnp.where(core == 0, far * nx + near, near * nx + far)
                        at = lax.rem(block + core * (count // 2), count)
                        ordered_ref[at, :, parity * columns : (parity + 1) * columns] = ref[p, i]
    line_at = lax.rem(y * nx + core * (count // 2), count)
    line_ref[...] = ordered_ref[pl.ds(line_at, nx)]
    rows = ordered_ref.shape[1]
    depth = nx * rows
    for which, factor_ref in enumerate((mine_ref, other_ref)):
        for k in range(ny // 2):
            rhs = ordered_ref[pl.ds((which * (ny // 2) + k) * nx, nx)]
            term = jnp.dot(
                factor_ref[:, k * depth : (k + 1) * depth],
                rhs.reshape(depth, 2 * columns),
                preferred_element_type=jnp.float32,
            )
            if which == 0 and k == 0:
                sum_ref[...] = term
            else:
                sum_ref[...] += term
    half_ref[...] = sum_ref[...].astype(jnp.bfloat16)


def half_transform(factors_mine, factors_other, arrivals):
    ny, nx = lax.axis_size(Y), lax.axis_size(X)
    rows, width = arrivals[0].shape[-2:]
    width *= 2
    vmem = pl.BlockSpec(memory_space=pltpu.VMEM)
    return pl.pallas_call(
        functools.partial(half_kernel, (ny, nx)),
        out_shape=(
            jax.ShapeDtypeStruct((factors_mine.shape[0], width), jnp.bfloat16),
            jax.ShapeDtypeStruct((nx, rows, width), jnp.bfloat16),
        ),
        in_specs=[vmem] * (2 + len(arrivals)),
        out_specs=(vmem, vmem),
        scratch_shapes=[
            pltpu.VMEM((ny * nx, rows, width), jnp.bfloat16),
            pltpu.VMEM((factors_mine.shape[0], width), jnp.float32),
        ],
        compiler_params=pltpu.CompilerParams(vmem_limit_bytes=40 << 20),
        cost_estimate=pl.CostEstimate(
            flops=4 * factors_mine.size * width, bytes_accessed=8 << 20, transcendentals=0
        ),
    )(factors_mine, factors_other, *arrivals)


def put(into, piece, index):
    return lax.dynamic_update_index_in_dim(into, piece, index, 0)


def gather_rows(own, axis, parity):
    n, me = lax.axis_size(axis), lax.axis_index(axis)
    into = put(jnp.zeros((n, *own.shape), own.dtype), own, me)
    slot = 1
    for arrived in ring_steps(own, lambda v, step: swap(v, axis, (parity + step) % 2), n):
        for piece in arrived:
            into = put(into, piece, source(slot, me, parity, n))
            slot += 1
    return into


def in_parts(value):
    parts = []
    for _ in range(3):
        part = lax.reduce_precision(value, 8, 7)
        parts.append(part)
        value = value - part
    return jnp.stack(parts, axis=-1).astype(jnp.bfloat16)


def tile_of(values, columns):
    flat = in_parts(values).reshape(-1)
    return jnp.pad(flat[None], ((0, TILE - 1), (0, columns - flat.size)))


def shards(factors, orbitals, field_term):
    aux_count, rows, half_n = factors.shape
    ny, nx = lax.axis_size(Y), lax.axis_size(X)
    core = lax.axis_index("col")

    flat = factors.reshape(aux_count * rows, half_n)
    flat_other = other_core(flat)
    width = orbitals.shape[1] // 2
    arrivals = []
    for parity in range(2):
        part = orbitals[:, parity * width : (parity + 1) * width]
        for stream in piece_streams(part, parity):
            arrivals += stream
    half, line = half_transform(flat, flat_other, arrivals)
    half = half.reshape(aux_count, rows, -1)
    gathered = []
    for aux in range(aux_count):
        along_y = gather_rows(half[aux], Y, aux % 2)
        along_x = gather_rows(half[aux], X, aux % 2)
        gathered.append((along_y.reshape(ny * rows, -1), along_x))

    def block_half(which):
        total = None
        for along_y, along_x in gathered:
            columns = lax.dynamic_slice_in_dim(along_x, which * (nx // 2), nx // 2, 0)
            term = lax.dot_general(
                along_y,
                columns.reshape(nx // 2 * rows, -1),
                (((1,), (1,)), ((), ())),
                preferred_element_type=jnp.float32,
            )
            total = term if total is None else total + term
        return total

    width = nx // 2 * rows
    arrived = other_core(block_half(1 - core).astype(jnp.bfloat16))
    total = block_half(core) + arrived.astype(jnp.float32)
    total = total.astype(jnp.bfloat16).reshape(ny, rows, width)

    fits = [
        jnp.sum(along_x.astype(jnp.float32) * line.astype(jnp.float32))
        for _, along_x in gathered
    ]
    tile = jnp.broadcast_to(tile_of(jnp.stack(fits), width), (ny, TILE, width))
    returned = lax.all_to_all(
        jnp.concatenate([total, tile], axis=1), Y, 0, 0, tiled=True
    )
    count = 3 * aux_count
    fitted = returned[:, rows, :count].astype(jnp.float32)
    fitted = fitted.reshape(ny, aux_count, 3).sum((0, 2))
    fitted = fitted + other_core(fitted)
    returned = returned[:, :rows].reshape(2, ny // 2, rows, width)
    kept = lax.dynamic_index_in_dim(returned, core, 0, False)
    swapped = other_core(lax.dynamic_index_in_dim(returned, 1 - core, 0, False))
    first = jnp.where(core == 0, kept, swapped)
    second = jnp.where(core == 0, swapped, kept)
    exchange = jnp.concatenate([first, second], axis=2)
    exchange = jnp.concatenate(list(exchange), axis=1)

    coulomb = jnp.zeros(field_term.shape, jnp.float32)
    for aux in range(aux_count):
        coulomb = coulomb + fitted[aux] * factors[aux].astype(jnp.float32)
    fock_matrix = (
        field_term.astype(jnp.float32) + coulomb - 0.25 * exchange.astype(jnp.float32)
    )
    return fock_matrix.astype(jnp.bfloat16)


def solution(mesh):
    side = math.isqrt(mesh.shape["row"])
    finer = Mesh(
        mesh.devices.reshape(mesh.shape["grp"], side, side, mesh.shape["col"]),
        ("grp", Y, X, "col"),
    )
    return jax.shard_map(
        shards,
        mesh=finer,
        in_specs=(P(None, GRP_ROW, "col"), P(GRP_ROW, "col"), P(GRP_ROW, "col")),
        out_specs=P(GRP_ROW, "col"),
        check_vma=False,
    )
```

```python
import functools
import math

import jax
import jax.numpy as jnp
from jax import lax
from jax.experimental import pallas as pl
from jax.experimental.pallas import tpu as pltpu
from jax.sharding import Mesh
from jax.sharding import PartitionSpec as P

GRP_ROW = ("grp", "row_0", "row_1")
Y, X = "row_0", "row_1"
TILE, LANES = 8, 128


def partner(i, n, parity):
    return i ^ 1 if parity == 0 else (((i + 1) ^ 1) - 1) % n


def swap(value, axis, parity):
    n = lax.axis_size(axis)
    return lax.ppermute(value, axis, [(i, partner(i, n, parity)) for i in range(n)])


def swap_by_core(value, parity, phase):
    ny, nx = lax.axis_size(Y), lax.axis_size(X)
    pairs = []
    for y in range(ny):
        for x in range(nx):
            for core in range(2):
                to_y, to_x = y, x
                if core == phase:
                    to_x = partner(x, nx, parity)
                else:
                    to_y = partner(y, ny, parity)
                pairs.append(((y * nx + x) * 2 + core, (to_y * nx + to_x) * 2 + core))
    return lax.ppermute(value, (Y, X, "col"), pairs)


def other_core(value):
    return lax.ppermute(value, "col", [(0, 1), (1, 0)])


def source(slot, me, parity, n):
    sign = 1 - 2 * lax.rem(me + parity, 2)
    pair = lax.div(slot, 2)
    side = 1 - 2 * lax.rem(pair, 2)
    offset = jnp.where(slot < 2, slot, side * (pair + lax.rem(slot, 2)))
    return lax.rem(me + sign * offset + n, n)


def ring_steps(own, exchange, n):
    held = exchange(own, 0)
    yield held[None]
    sent = jnp.stack([own, held])
    for step in range(1, n // 2):
        sent = exchange(sent, step)
        yield sent


def piece_streams(part, parity):
    n = lax.axis_size(X)

    def phase(which):
        return lambda value, step: swap_by_core(value, (parity + step) % 2, which)

    steps = list(ring_steps(part, phase(0), n))
    lines = (
        jnp.concatenate([part[None], *steps[: n // 4]]),
        jnp.concatenate(steps[n // 4 :]),
    )
    return [(line[None], *ring_steps(line, phase(1), n)) for line in lines]


def half_kernel(shape, mine_ref, other_ref, *refs):
    half_ref, line_ref, ordered_ref, sum_ref = refs[-4:]
    arrivals = list(refs[:-4])
    y, x, core = lax.axis_index(Y), lax.axis_index(X), lax.axis_index("col")
    ny, nx = shape
    n, count = nx, ny * nx
    major, minor = jnp.where(core == 0, y, x), jnp.where(core == 0, x, y)
    columns = arrivals[0].shape[-1]
    for parity in range(2):
        for first_near in (0, n // 2):
            slot = 0
            while slot < n:
                ref = arrivals.pop(0)
                for p in range(ref.shape[0]):
                    far = source(slot, major, parity, n)
                    slot += 1
                    for i in range(n // 2):
                        near = source(first_near + i, minor, parity, n)
                        block = jnp.where(core == 0, far * nx + near, near * nx + far)
                        at = lax.rem(block + core * (count // 2), count)
                        ordered_ref[at, :, parity * columns : (parity + 1) * columns] = ref[p, i]
    line_at = lax.rem(y * nx + core * (count // 2), count)
    line_ref[...] = ordered_ref[pl.ds(line_at, nx)]
    rows = ordered_ref.shape[1]
    depth = nx * rows
    for which, factor_ref in enumerate((mine_ref, other_ref)):
        for k in range(ny // 2):
            rhs = ordered_ref[pl.ds((which * (ny // 2) + k) * nx, nx)]
            term = jnp.dot(
                factor_ref[:, k * depth : (k + 1) * depth],
                rhs.reshape(depth, 2 * columns),
                preferred_element_type=jnp.float32,
            )
            if which == 0 and k == 0:
                sum_ref[...] = term
            else:
                sum_ref[...] += term
    half_ref[...] = sum_ref[...].astype(jnp.bfloat16)


def half_transform(factors_mine, factors_other, arrivals):
    ny, nx = lax.axis_size(Y), lax.axis_size(X)
    rows, width = arrivals[0].shape[-2:]
    width *= 2
    return local_call(
        functools.partial(half_kernel, (ny, nx)),
        (
            jax.ShapeDtypeStruct((factors_mine.shape[0], width), jnp.bfloat16),
            jax.ShapeDtypeStruct((nx, rows, width), jnp.bfloat16),
        ),
        (factors_mine, factors_other, *arrivals),
        4 * factors_mine.size * width,
        (
            pltpu.VMEM((ny * nx, rows, width), jnp.bfloat16),
            pltpu.VMEM((factors_mine.shape[0], width), jnp.float32),
        ),
    )


def row_pieces(own, axis, parity):
    n = lax.axis_size(axis)
    return [
        own[None],
        *ring_steps(own, lambda v, step: swap(v, axis, (parity + step) % 2), n),
    ]


def local_call(kernel, outs, args, flops, scratch=(), limit=24 << 20):
    vmem = pl.BlockSpec(memory_space=pltpu.VMEM)
    many = isinstance(outs, tuple)
    return pl.pallas_call(
        kernel,
        out_shape=outs,
        in_specs=[vmem] * len(args),
        out_specs=(vmem,) * len(outs) if many else vmem,
        scratch_shapes=scratch,
        compiler_params=pltpu.CompilerParams(vmem_limit_bytes=limit),
        cost_estimate=pl.CostEstimate(
            flops=flops, bytes_accessed=sum(2 * a.size for a in args), transcendentals=0
        ),
    )(*args)


def block_dot(rows, columns):
    return lax.dot_general(
        rows, columns, (((1,), (1,)), ((), ())), preferred_element_type=jnp.float32
    )


def theirs_kernel(n, aux_count, *refs):
    along_x_ref, along_y_ref, theirs_ref = refs[-3:]
    pieces = list(refs[:-3])
    y, x, core = lax.axis_index(Y), lax.axis_index(X), lax.axis_index("col")
    width = pieces[0].shape[-1]
    for aux in range(aux_count):
        for into_ref, me, shift in ((along_y_ref, y, 0), (along_x_ref, x, core * (n // 2))):
            slot = 0
            while slot < n:
                ref = pieces.pop(0)
                for p in range(ref.shape[0]):
                    at = lax.rem(source(slot, me, aux % 2, n) + shift, n)
                    into_ref[at, :, aux * width : (aux + 1) * width] = ref[p]
                    slot += 1
    depth = along_x_ref.shape[2]
    columns = along_x_ref[n // 2 :].reshape(-1, depth)
    for k in range(2):
        part = along_y_ref[k * (n // 2) : (k + 1) * (n // 2)].reshape(-1, depth)
        theirs_ref[k * part.shape[0] : (k + 1) * part.shape[0]] = block_dot(
            part, columns
        ).astype(jnp.bfloat16)


def split_parts(value):
    parts = []
    for _ in range(3):
        part = value.astype(jnp.bfloat16).astype(jnp.float32)
        parts.append(part)
        value = value - part
    return parts


def mine_kernel(n, aux_count, along_x_ref, along_y_ref, line_ref, mine_ref, tile_ref):
    core = lax.axis_index("col")
    depth = along_x_ref.shape[2]
    width = depth // aux_count
    columns = along_x_ref[: n // 2].reshape(-1, depth)
    for k in range(2):
        part = along_y_ref[k * (n // 2) : (k + 1) * (n // 2)].reshape(-1, depth)
        mine_ref[k * part.shape[0] : (k + 1) * part.shape[0]] = block_dot(part, columns)
    lane = lax.broadcasted_iota(jnp.int32, tile_ref.shape, 1)
    tile = jnp.zeros(tile_ref.shape, jnp.float32)
    for aux in range(aux_count):
        total = jnp.zeros(along_x_ref.shape[1:2] + (width,), jnp.float32)
        for i in range(n):
            at = lax.rem(i + core * (n // 2), n)
            total += along_x_ref[at, :, aux * width : (aux + 1) * width].astype(
                jnp.float32
            ) * line_ref[i].astype(jnp.float32)
        total = jnp.sum(jnp.sum(total, axis=0, keepdims=True), axis=1, keepdims=True)
        wide = jnp.broadcast_to(total, tile_ref.shape)
        for p, part in enumerate(split_parts(wide)):
            tile = jnp.where(lane == 3 * aux + p, part, tile)
    tile_ref[...] = tile.astype(jnp.bfloat16)


def pack_kernel(mine_ref, arrived_ref, tile_ref, out_ref):
    n, rows = out_ref.shape[0], out_ref.shape[1] - TILE
    for i in range(n):
        at = slice(i * rows, (i + 1) * rows)
        total = mine_ref[at] + arrived_ref[at].astype(jnp.float32)
        out_ref[i, :rows] = total.astype(jnp.bfloat16)
        out_ref[i, rows:] = tile_ref[...]


def split_kernel(returned_ref, out_ref):
    core = lax.axis_index("col")
    half, rows = out_ref.shape[0], out_ref.shape[1] - TILE
    for k in range(half):
        out_ref[k, :rows] = returned_ref[(1 - core) * half + k, :rows]
        out_ref[k, rows:] = jnp.zeros((TILE, out_ref.shape[2]), out_ref.dtype)
        out_ref[k, rows:, :LANES] = returned_ref[k, rows:, :LANES]
        out_ref[k, rows:, LANES : 2 * LANES] = returned_ref[half + k, rows:, :LANES]


def final_kernel(aux_count, returned_ref, swapped_ref, factor_ref, field_ref, out_ref):
    core = lax.axis_index("col")
    step = pl.program_id(0)
    half, rows = swapped_ref.shape[0], out_ref.shape[0]
    width = returned_ref.shape[2]
    tiles = jnp.zeros((TILE, LANES), jnp.float32)
    for k in range(2 * half):
        tiles += returned_ref[k, rows:, :LANES].astype(jnp.float32)
    for k in range(half):
        tiles += swapped_ref[k, rows:, :LANES].astype(jnp.float32)
        tiles += swapped_ref[k, rows:, LANES : 2 * LANES].astype(jnp.float32)
    lane = lax.broadcasted_iota(jnp.int32, tiles.shape, 1)
    kept = returned_ref[core * half + step, :rows].astype(jnp.float32)
    swapped = swapped_ref[step, :rows].astype(jnp.float32)
    halves = (jnp.where(core == 0, kept, swapped), jnp.where(core == 0, swapped, kept))
    gammas = []
    for aux in range(aux_count):
        picked = jnp.where((lane >= 3 * aux) & (lane < 3 * aux + 3), tiles, 0.0)
        gammas.append(jnp.sum(picked[:1], axis=1, keepdims=True))
    for which, exchange in enumerate(halves):
        at = slice(which * width, (which + 1) * width)
        coulomb = jnp.zeros(exchange.shape, jnp.float32)
        for aux in range(aux_count):
            coulomb += gammas[aux] * factor_ref[aux, :, at].astype(jnp.float32)
        fock = field_ref[:, at].astype(jnp.float32) + coulomb - 0.25 * exchange
        out_ref[:, at] = fock.astype(jnp.bfloat16)


def shards(factors, orbitals, field_term):
    aux_count, rows, half_n = factors.shape
    n = lax.axis_size(X)

    flat = factors.reshape(aux_count * rows, half_n)
    flat_other = other_core(flat)
    width = orbitals.shape[1] // 2
    arrivals = []
    for parity in range(2):
        part = orbitals[:, parity * width : (parity + 1) * width]
        for stream in piece_streams(part, parity):
            arrivals += stream
    half, line = half_transform(flat, flat_other, arrivals)
    half = half.reshape(aux_count, rows, -1)

    pieces = []
    for aux in range(aux_count):
        for axis in (Y, X):
            pieces += row_pieces(half[aux], axis, aux % 2)
    depth = aux_count * half.shape[2]
    width = n // 2 * rows
    ordered = jax.ShapeDtypeStruct((n, rows, depth), jnp.bfloat16)
    along_x, along_y, theirs = local_call(
        functools.partial(theirs_kernel, n, aux_count),
        (ordered, ordered, jax.ShapeDtypeStruct((n * rows, width), jnp.bfloat16)),
        pieces,
        2 * n * rows * width * depth,
    )
    arrived = other_core(theirs)
    mine, tile = local_call(
        functools.partial(mine_kernel, n, aux_count),
        (
            jax.ShapeDtypeStruct((n * rows, width), jnp.float32),
            jax.ShapeDtypeStruct((TILE, width), jnp.bfloat16),
        ),
        (along_x, along_y, line),
        2 * n * rows * width * depth,
    )
    packed = local_call(
        pack_kernel,
        jax.ShapeDtypeStruct((n, rows + TILE, width), jnp.bfloat16),
        (mine, arrived, tile),
        n * rows * width,
    )
    returned = lax.all_to_all(packed, Y, 0, 0, tiled=True)
    given = local_call(
        split_kernel,
        jax.ShapeDtypeStruct((n // 2, rows + TILE, width), jnp.bfloat16),
        (returned,),
        n * rows * width,
    )
    swapped = other_core(given)
    whole = pl.BlockSpec(memory_space=pltpu.VMEM)
    return pl.pallas_call(
        functools.partial(final_kernel, aux_count),
        grid=(n // 2,),
        out_shape=jax.ShapeDtypeStruct(field_term.shape, jnp.bfloat16),
        in_specs=[
            whole,
            whole,
            pl.BlockSpec((aux_count, rows, 2 * width), lambda k: (0, 0, k)),
            pl.BlockSpec((rows, 2 * width), lambda k: (0, k)),
        ],
        out_specs=pl.BlockSpec((rows, 2 * width), lambda k: (0, k)),
        compiler_params=pltpu.CompilerParams(vmem_limit_bytes=24 << 20),
        cost_estimate=pl.CostEstimate(
            flops=8 * field_term.size, bytes_accessed=8 * field_term.size, transcendentals=0
        ),
    )(returned, swapped, factors, field_term)


def solution(mesh):
    side = math.isqrt(mesh.shape["row"])
    finer = Mesh(
        mesh.devices.reshape(mesh.shape["grp"], side, side, mesh.shape["col"]),
        ("grp", Y, X, "col"),
    )
    return jax.shard_map(
        shards,
        mesh=finer,
        in_specs=(P(None, GRP_ROW, "col"), P(GRP_ROW, "col"), P(GRP_ROW, "col")),
        out_specs=P(GRP_ROW, "col"),
        check_vma=False,
    )
```

```python
import functools
import math

import jax
import jax.numpy as jnp
from jax import lax
from jax.experimental import pallas as pl
from jax.experimental.pallas import tpu as pltpu
from jax.sharding import Mesh
from jax.sharding import PartitionSpec as P

GRP_ROW = ("grp", "row_0", "row_1")
Y, X = "row_0", "row_1"
TILE, LANES = 8, 128


def partner(i, n, parity):
    return i ^ 1 if parity == 0 else (((i + 1) ^ 1) - 1) % n


def swap(value, axis, parity):
    n = lax.axis_size(axis)
    return lax.ppermute(value, axis, [(i, partner(i, n, parity)) for i in range(n)])


def swap_by_core(value, parity, phase):
    ny, nx = lax.axis_size(Y), lax.axis_size(X)
    pairs = []
    for y in range(ny):
        for x in range(nx):
            for core in range(2):
                to_y, to_x = y, x
                if core == phase:
                    to_x = partner(x, nx, parity)
                else:
                    to_y = partner(y, ny, parity)
                pairs.append(((y * nx + x) * 2 + core, (to_y * nx + to_x) * 2 + core))
    return lax.ppermute(value, (Y, X, "col"), pairs)


def other_core(value):
    return lax.ppermute(value, "col", [(0, 1), (1, 0)])


def source(slot, me, parity, n):
    sign = 1 - 2 * lax.rem(me + parity, 2)
    pair = lax.div(slot, 2)
    side = 1 - 2 * lax.rem(pair, 2)
    offset = jnp.where(slot < 2, slot, side * (pair + lax.rem(slot, 2)))
    return lax.rem(me + sign * offset + n, n)


def ring_steps(own, exchange, n):
    held = exchange(own, 0)
    yield held[None]
    sent = jnp.stack([own, held])
    for step in range(1, n // 2):
        sent = exchange(sent, step)
        yield sent


def piece_streams(part, parity):
    n = lax.axis_size(X)

    def phase(which):
        return lambda value, step: swap_by_core(value, (parity + step) % 2, which)

    steps = list(ring_steps(part, phase(0), n))
    lines = (
        jnp.concatenate([part[None], *steps[: n // 4]]),
        jnp.concatenate(steps[n // 4 :]),
    )
    return [(line[None], *ring_steps(line, phase(1), n)) for line in lines]


def return_groups():
    ny, nx = lax.axis_size(Y), lax.axis_size(X)

    def at(y, x, core):
        return (y * nx + x) * 2 + core

    columns = [[at(y, x, 0) for y in range(ny)] for x in range(nx)]
    return columns + [[at(y, x, 1) for x in range(nx)] for y in range(ny)]


def half_kernel(shape, mine_ref, other_ref, *refs):
    half_ref, line_ref, ordered_ref, sum_ref = refs[-4:]
    arrivals = list(refs[:-4])
    y, x, core = lax.axis_index(Y), lax.axis_index(X), lax.axis_index("col")
    ny, nx = shape
    n, count = nx, ny * nx
    major, minor = jnp.where(core == 0, y, x), jnp.where(core == 0, x, y)
    columns = arrivals[0].shape[-1]
    for parity in range(2):
        for first_near in (0, n // 2):
            slot = 0
            while slot < n:
                ref = arrivals.pop(0)
                for p in range(ref.shape[0]):
                    far = source(slot, major, parity, n)
                    slot += 1
                    for i in range(n // 2):
                        near = source(first_near + i, minor, parity, n)
                        block = jnp.where(core == 0, far * nx + near, near * nx + far)
                        at = lax.rem(block + core * (count // 2), count)
                        ordered_ref[at, :, parity * columns : (parity + 1) * columns] = ref[p, i]
    for i in range(n):
        block = jnp.where(core == 0, y * nx + i, i * nx + x)
        line_ref[i] = ordered_ref[lax.rem(block + core * (count // 2), count)]
    rows = ordered_ref.shape[1]
    depth = nx * rows
    for which, factor_ref in enumerate((mine_ref, other_ref)):
        for k in range(ny // 2):
            rhs = ordered_ref[pl.ds((which * (ny // 2) + k) * nx, nx)]
            term = jnp.dot(
                factor_ref[:, k * depth : (k + 1) * depth],
                rhs.reshape(depth, 2 * columns),
                preferred_element_type=jnp.float32,
            )
            if which == 0 and k == 0:
                sum_ref[...] = term
            else:
                sum_ref[...] += term
    half_ref[...] = sum_ref[...].astype(jnp.bfloat16)


def half_transform(factors_mine, factors_other, arrivals):
    ny, nx = lax.axis_size(Y), lax.axis_size(X)
    rows, width = arrivals[0].shape[-2:]
    width *= 2
    return local_call(
        functools.partial(half_kernel, (ny, nx)),
        (
            jax.ShapeDtypeStruct((factors_mine.shape[0], width), jnp.bfloat16),
            jax.ShapeDtypeStruct((nx, rows, width), jnp.bfloat16),
        ),
        (factors_mine, factors_other, *arrivals),
        4 * factors_mine.size * width,
        (
            pltpu.VMEM((ny * nx, rows, width), jnp.bfloat16),
            pltpu.VMEM((factors_mine.shape[0], width), jnp.float32),
        ),
    )


def row_pieces(own, axis, parity):
    n = lax.axis_size(axis)
    return [
        own[None],
        *ring_steps(own, lambda v, step: swap(v, axis, (parity + step) % 2), n),
    ]


def local_call(kernel, outs, args, flops, scratch=(), limit=24 << 20):
    vmem = pl.BlockSpec(memory_space=pltpu.VMEM)
    many = isinstance(outs, tuple)
    return pl.pallas_call(
        kernel,
        out_shape=outs,
        in_specs=[vmem] * len(args),
        out_specs=(vmem,) * len(outs) if many else vmem,
        scratch_shapes=scratch,
        compiler_params=pltpu.CompilerParams(vmem_limit_bytes=limit),
        cost_estimate=pl.CostEstimate(
            flops=flops, bytes_accessed=sum(2 * a.size for a in args), transcendentals=0
        ),
    )(*args)


def block_dot(rows, columns):
    return lax.dot_general(
        rows, columns, (((1,), (1,)), ((), ())), preferred_element_type=jnp.float32
    )


def half_block(n, along_ref, which, put):
    y, x = lax.axis_index(Y), lax.axis_index(X)
    far = lax.div(jnp.where(which == 0, y, x), n // 2)
    first = jnp.where(which == 0, far, 1 - far) * (n // 2)
    depth = along_ref.shape[3]
    columns = along_ref[which, pl.ds(first, n // 2)].reshape(-1, depth)
    for k in range(2):
        part = along_ref[1 - which, k * (n // 2) : (k + 1) * (n // 2)].reshape(-1, depth)
        put(slice(k * part.shape[0], (k + 1) * part.shape[0]), block_dot(part, columns))


def theirs_kernel(n, aux_count, *refs):
    along_ref, theirs_ref = refs[-2:]
    pieces = list(refs[:-2])
    y, x, core = lax.axis_index(Y), lax.axis_index(X), lax.axis_index("col")
    width = pieces[0].shape[-1]
    for aux in range(aux_count):
        for which, me in ((1, y), (0, x)):
            slot = 0
            while slot < n:
                ref = pieces.pop(0)
                for p in range(ref.shape[0]):
                    at = source(slot, me, aux % 2, n)
                    along_ref[which, at, :, aux * width : (aux + 1) * width] = ref[p]
                    slot += 1

    def put(at, value):
        theirs_ref[at] = value.astype(jnp.bfloat16)

    half_block(n, along_ref, 1 - core, put)


def split_parts(value):
    parts = []
    for _ in range(3):
        part = value.astype(jnp.bfloat16).astype(jnp.float32)
        parts.append(part)
        value = value - part
    return parts


def mine_kernel(n, aux_count, along_ref, line_ref, mine_ref, tile_ref):
    core = lax.axis_index("col")
    width = along_ref.shape[3] // aux_count

    def put(at, value):
        mine_ref[at] = value

    half_block(n, along_ref, core, put)
    lane = lax.broadcasted_iota(jnp.int32, tile_ref.shape, 1)
    tile = jnp.zeros(tile_ref.shape, jnp.float32)
    for aux in range(aux_count):
        total = jnp.zeros(along_ref.shape[2:3] + (width,), jnp.float32)
        for i in range(n):
            total += along_ref[core, i, :, aux * width : (aux + 1) * width].astype(
                jnp.float32
            ) * line_ref[i].astype(jnp.float32)
        total = jnp.sum(jnp.sum(total, axis=0, keepdims=True), axis=1, keepdims=True)
        wide = jnp.broadcast_to(total, tile_ref.shape)
        for p, part in enumerate(split_parts(wide)):
            tile = jnp.where(lane == 3 * aux + p, part, tile)
    tile_ref[...] = tile.astype(jnp.bfloat16)


def pack_kernel(mine_ref, arrived_ref, tile_ref, out_ref):
    n, rows = out_ref.shape[0], out_ref.shape[1] - TILE
    for i in range(n):
        at = slice(i * rows, (i + 1) * rows)
        total = mine_ref[at] + arrived_ref[at].astype(jnp.float32)
        out_ref[i, :rows] = total.astype(jnp.bfloat16)
        out_ref[i, rows:] = tile_ref[...]


def split_kernel(returned_ref, out_ref):
    half, rows = out_ref.shape[0], out_ref.shape[1] - TILE
    for k in range(half):
        out_ref[k] = returned_ref[half + k]
        out_ref[k, rows:, LANES : 2 * LANES] = returned_ref[k, rows:, :LANES]


def final_kernel(aux_count, returned_ref, swapped_ref, factor_ref, field_ref, out_ref, joined_ref):
    core = lax.axis_index("col")
    half, rows = swapped_ref.shape[0], out_ref.shape[0]
    width = returned_ref.shape[2]
    tiles = jnp.zeros((TILE, LANES), jnp.float32)
    for k in range(2 * half):
        tiles += returned_ref[k, rows:, :LANES].astype(jnp.float32)
    for k in range(half):
        tiles += swapped_ref[k, rows:, :LANES].astype(jnp.float32)
        tiles += swapped_ref[k, rows:, LANES : 2 * LANES].astype(jnp.float32)
    lane = lax.broadcasted_iota(jnp.int32, tiles.shape, 1)
    gammas = []
    for aux in range(aux_count):
        picked = jnp.where((lane >= 3 * aux) & (lane < 3 * aux + 3), tiles, 0.0)
        gammas.append(jnp.sum(picked[:1], axis=1, keepdims=True))
    for j in range(half):
        piece = jnp.where(core == 0, swapped_ref[j, :rows], returned_ref[j, :rows])
        for k in range(half):
            joined_ref[k, :, j * rows : (j + 1) * rows] = piece[:, k * rows : (k + 1) * rows]
    for k in range(half):
        straight = jnp.where(core == 0, returned_ref[k, :rows], swapped_ref[k, :rows])
        joined = joined_ref[k]
        sides = (jnp.where(core == 0, straight, joined), jnp.where(core == 0, joined, straight))
        for which, exchange in enumerate(sides):
            at = slice((2 * k + which) * width, (2 * k + which + 1) * width)
            coulomb = jnp.zeros(exchange.shape, jnp.float32)
            for aux in range(aux_count):
                coulomb += gammas[aux] * factor_ref[aux, :, at].astype(jnp.float32)
            fock = field_ref[:, at].astype(jnp.float32) + coulomb
            out_ref[:, at] = (fock - 0.25 * exchange.astype(jnp.float32)).astype(jnp.bfloat16)


def shards(factors, orbitals, field_term):
    aux_count, rows, half_n = factors.shape
    n = lax.axis_size(X)

    flat = factors.reshape(aux_count * rows, half_n)
    flat_other = other_core(flat)
    width = orbitals.shape[1] // 2
    arrivals = []
    for parity in range(2):
        part = orbitals[:, parity * width : (parity + 1) * width]
        for stream in piece_streams(part, parity):
            arrivals += stream
    half, line = half_transform(flat, flat_other, arrivals)
    half = half.reshape(aux_count, rows, -1)

    pieces = []
    for aux in range(aux_count):
        for axis in (Y, X):
            pieces += row_pieces(half[aux], axis, aux % 2)
    depth = aux_count * half.shape[2]
    width = n // 2 * rows
    along, theirs = local_call(
        functools.partial(theirs_kernel, n, aux_count),
        (
            jax.ShapeDtypeStruct((2, n, rows, depth), jnp.bfloat16),
            jax.ShapeDtypeStruct((n * rows, width), jnp.bfloat16),
        ),
        pieces,
        2 * n * rows * width * depth,
    )
    arrived = other_core(theirs)
    mine, tile = local_call(
        functools.partial(mine_kernel, n, aux_count),
        (
            jax.ShapeDtypeStruct((n * rows, width), jnp.float32),
            jax.ShapeDtypeStruct((TILE, width), jnp.bfloat16),
        ),
        (along, line),
        2 * n * rows * width * depth,
    )
    packed = local_call(
        pack_kernel,
        jax.ShapeDtypeStruct((n, rows + TILE, width), jnp.bfloat16),
        (mine, arrived, tile),
        n * rows * width,
    )
    returned = lax.all_to_all(
        packed, (Y, X, "col"), 0, 0, axis_index_groups=return_groups(), tiled=True
    )
    given = local_call(
        split_kernel,
        jax.ShapeDtypeStruct((n // 2, rows + TILE, width), jnp.bfloat16),
        (returned,),
        n * rows * width,
    )
    swapped = other_core(given)
    return local_call(
        functools.partial(final_kernel, aux_count),
        jax.ShapeDtypeStruct(field_term.shape, jnp.bfloat16),
        (returned, swapped, factors, field_term),
        8 * field_term.size,
        (pltpu.VMEM((n // 2, rows, width), jnp.bfloat16),),
    )


def solution(mesh):
    side = math.isqrt(mesh.shape["row"])
    finer = Mesh(
        mesh.devices.reshape(mesh.shape["grp"], side, side, mesh.shape["col"]),
        ("grp", Y, X, "col"),
    )
    return jax.shard_map(
        shards,
        mesh=finer,
        in_specs=(P(None, GRP_ROW, "col"), P(GRP_ROW, "col"), P(GRP_ROW, "col")),
        out_specs=P(GRP_ROW, "col"),
        check_vma=False,
    )
```

```python
import functools
import math

import jax
import jax.numpy as jnp
from jax import lax
from jax.experimental import pallas as pl
from jax.experimental.pallas import tpu as pltpu
from jax.sharding import Mesh
from jax.sharding import PartitionSpec as P

GRP_ROW = ("grp", "row_0", "row_1")
Y, X = "row_0", "row_1"
TILE, LANES = 8, 128


def partner(i, n, parity):
    return i ^ 1 if parity == 0 else (((i + 1) ^ 1) - 1) % n


def swap(value, axis, parity):
    n = lax.axis_size(axis)
    return lax.ppermute(value, axis, [(i, partner(i, n, parity)) for i in range(n)])


def swap_by_core(value, parity, phase):
    ny, nx = lax.axis_size(Y), lax.axis_size(X)
    pairs = []
    for y in range(ny):
        for x in range(nx):
            for core in range(2):
                to_y, to_x = y, x
                if core == phase:
                    to_x = partner(x, nx, parity)
                else:
                    to_y = partner(y, ny, parity)
                pairs.append(((y * nx + x) * 2 + core, (to_y * nx + to_x) * 2 + core))
    return lax.ppermute(value, (Y, X, "col"), pairs)


def other_core(value):
    return lax.ppermute(value, "col", [(0, 1), (1, 0)])


def source(slot, me, parity, n):
    sign = 1 - 2 * lax.rem(me + parity, 2)
    pair = lax.div(slot, 2)
    side = 1 - 2 * lax.rem(pair, 2)
    offset = jnp.where(slot < 2, slot, side * (pair + lax.rem(slot, 2)))
    return lax.rem(me + sign * offset + n, n)


def ring_steps(own, exchange, n):
    held = exchange(own, 0)
    yield held[None]
    sent = jnp.stack([own, held])
    for step in range(1, n // 2):
        sent = exchange(sent, step)
        yield sent


def core_groups(first):
    ny, nx = lax.axis_size(Y), lax.axis_size(X)

    def at(y, x, core):
        return (y * nx + x) * 2 + core

    rows = [[at(y, x, first) for x in range(nx)] for y in range(ny)]
    return rows + [[at(y, x, 1 - first) for y in range(ny)] for x in range(nx)]


def piece_streams(orbitals):
    n = lax.axis_size(X)
    rows, columns = orbitals.shape
    line = lax.all_to_all(
        jnp.broadcast_to(orbitals, (n, rows, columns)),
        (Y, X, "col"),
        0,
        0,
        axis_index_groups=core_groups(0),
        tiled=True,
    )
    arrivals, places = [], []
    for parity in range(2):
        part = line[:, :, parity * (columns // 2) : (parity + 1) * (columns // 2)]
        held = swap_by_core(part, parity, 1)
        arrivals += [part[None], held[None]]
        places += [(parity, 0, 0), (parity, 1, 0)]
        for which in range(2):
            first = which * (n // 2)
            half = slice(first, first + n // 2)
            sent = jnp.stack([part[half], held[half]])
            for step in range(1, n // 2):
                sent = swap_by_core(sent, (parity + step) % 2, 1)
                arrivals.append(sent)
                places.append((parity, 2 * step, first))
    return arrivals, places


def half_kernel(shape, places, mine_ref, other_ref, *refs):
    half_ref, line_ref, ordered_ref, sum_ref = refs[-4:]
    arrivals = list(refs[:-4])
    y, x, core = lax.axis_index(Y), lax.axis_index(X), lax.axis_index("col")
    ny, nx = shape
    n, count = nx, ny * nx
    major = jnp.where(core == 0, y, x)
    columns = arrivals[0].shape[-1]
    for (parity, first_slot, first_near), ref in zip(places, arrivals):
        for p in range(ref.shape[0]):
            far = source(first_slot + p, major, parity, n)
            for i in range(ref.shape[1]):
                near = first_near + i
                block = jnp.where(core == 0, far * nx + near, near * nx + far)
                at = lax.rem(block + core * (count // 2), count)
                ordered_ref[at, :, parity * columns : (parity + 1) * columns] = ref[p, i]
    for i in range(n):
        block = jnp.where(core == 0, y * nx + i, i * nx + x)
        line_ref[i] = ordered_ref[lax.rem(block + core * (count // 2), count)]
    rows = ordered_ref.shape[1]
    depth = nx * rows
    for which, factor_ref in enumerate((mine_ref, other_ref)):
        for k in range(ny // 2):
            rhs = ordered_ref[pl.ds((which * (ny // 2) + k) * nx, nx)]
            term = jnp.dot(
                factor_ref[:, k * depth : (k + 1) * depth],
                rhs.reshape(depth, 2 * columns),
                preferred_element_type=jnp.float32,
            )
            if which == 0 and k == 0:
                sum_ref[...] = term
            else:
                sum_ref[...] += term
    half_ref[...] = sum_ref[...].astype(jnp.bfloat16)


def half_transform(factors_mine, factors_other, arrivals, places):
    ny, nx = lax.axis_size(Y), lax.axis_size(X)
    rows, width = arrivals[0].shape[-2:]
    width *= 2
    return local_call(
        functools.partial(half_kernel, (ny, nx), places),
        (
            jax.ShapeDtypeStruct((factors_mine.shape[0], width), jnp.bfloat16),
            jax.ShapeDtypeStruct((nx, rows, width), jnp.bfloat16),
        ),
        (factors_mine, factors_other, *arrivals),
        4 * factors_mine.size * width,
        (
            pltpu.VMEM((ny * nx, rows, width), jnp.bfloat16),
            pltpu.VMEM((factors_mine.shape[0], width), jnp.float32),
        ),
    )


def row_pieces(own, axis, parity):
    n = lax.axis_size(axis)
    return [
        own[None],
        *ring_steps(own, lambda v, step: swap(v, axis, (parity + step) % 2), n),
    ]


def local_call(kernel, outs, args, flops, scratch=(), limit=24 << 20):
    vmem = pl.BlockSpec(memory_space=pltpu.VMEM)
    many = isinstance(outs, tuple)
    return pl.pallas_call(
        kernel,
        out_shape=outs,
        in_specs=[vmem] * len(args),
        out_specs=(vmem,) * len(outs) if many else vmem,
        scratch_shapes=scratch,
        compiler_params=pltpu.CompilerParams(vmem_limit_bytes=limit),
        cost_estimate=pl.CostEstimate(
            flops=flops, bytes_accessed=sum(2 * a.size for a in args), transcendentals=0
        ),
    )(*args)


def block_dot(rows, columns):
    return lax.dot_general(
        rows, columns, (((1,), (1,)), ((), ())), preferred_element_type=jnp.float32
    )


def half_block(n, along_ref, which, put):
    y, x = lax.axis_index(Y), lax.axis_index(X)
    far = lax.div(jnp.where(which == 0, y, x), n // 2)
    first = jnp.where(which == 0, far, 1 - far) * (n // 2)
    depth = along_ref.shape[3]
    columns = along_ref[which, pl.ds(first, n // 2)].reshape(-1, depth)
    for k in range(2):
        part = along_ref[1 - which, k * (n // 2) : (k + 1) * (n // 2)].reshape(-1, depth)
        put(slice(k * part.shape[0], (k + 1) * part.shape[0]), block_dot(part, columns))


def theirs_kernel(n, aux_count, *refs):
    along_ref, theirs_ref = refs[-2:]
    pieces = list(refs[:-2])
    y, x, core = lax.axis_index(Y), lax.axis_index(X), lax.axis_index("col")
    width = pieces[0].shape[-1]
    for aux in range(aux_count):
        for which, me in ((1, y), (0, x)):
            slot = 0
            while slot < n:
                ref = pieces.pop(0)
                for p in range(ref.shape[0]):
                    at = source(slot, me, aux % 2, n)
                    along_ref[which, at, :, aux * width : (aux + 1) * width] = ref[p]
                    slot += 1

    def put(at, value):
        theirs_ref[at] = value.astype(jnp.bfloat16)

    half_block(n, along_ref, 1 - core, put)


def split_parts(value):
    parts = []
    for _ in range(3):
        part = value.astype(jnp.bfloat16).astype(jnp.float32)
        parts.append(part)
        value = value - part
    return parts


def mine_kernel(n, aux_count, along_ref, line_ref, mine_ref, tile_ref):
    core = lax.axis_index("col")
    width = along_ref.shape[3] // aux_count

    def put(at, value):
        mine_ref[at] = value

    half_block(n, along_ref, core, put)
    lane = lax.broadcasted_iota(jnp.int32, tile_ref.shape, 1)
    tile = jnp.zeros(tile_ref.shape, jnp.float32)
    for aux in range(aux_count):
        total = jnp.zeros(along_ref.shape[2:3] + (width,), jnp.float32)
        for i in range(n):
            total += along_ref[core, i, :, aux * width : (aux + 1) * width].astype(
                jnp.float32
            ) * line_ref[i].astype(jnp.float32)
        total = jnp.sum(jnp.sum(total, axis=0, keepdims=True), axis=1, keepdims=True)
        wide = jnp.broadcast_to(total, tile_ref.shape)
        for p, part in enumerate(split_parts(wide)):
            tile = jnp.where(lane == 3 * aux + p, part, tile)
    tile_ref[...] = tile.astype(jnp.bfloat16)


def pack_kernel(mine_ref, arrived_ref, tile_ref, out_ref):
    n, rows = out_ref.shape[0], out_ref.shape[1] - TILE
    for i in range(n):
        at = slice(i * rows, (i + 1) * rows)
        total = mine_ref[at] + arrived_ref[at].astype(jnp.float32)
        out_ref[i, :rows] = total.astype(jnp.bfloat16)
        out_ref[i, rows:] = tile_ref[...]


def split_kernel(returned_ref, out_ref):
    half, rows = out_ref.shape[0], out_ref.shape[1] - TILE
    for k in range(half):
        out_ref[k] = returned_ref[half + k]
        out_ref[k, rows:, LANES : 2 * LANES] = returned_ref[k, rows:, :LANES]


def final_kernel(aux_count, returned_ref, swapped_ref, factor_ref, field_ref, out_ref, joined_ref):
    core = lax.axis_index("col")
    half, rows = swapped_ref.shape[0], out_ref.shape[0]
    width = returned_ref.shape[2]
    tiles = jnp.zeros((TILE, LANES), jnp.float32)
    for k in range(2 * half):
        tiles += returned_ref[k, rows:, :LANES].astype(jnp.float32)
    for k in range(half):
        tiles += swapped_ref[k, rows:, :LANES].astype(jnp.float32)
        tiles += swapped_ref[k, rows:, LANES : 2 * LANES].astype(jnp.float32)
    lane = lax.broadcasted_iota(jnp.int32, tiles.shape, 1)
    gammas = []
    for aux in range(aux_count):
        picked = jnp.where((lane >= 3 * aux) & (lane < 3 * aux + 3), tiles, 0.0)
        gammas.append(jnp.sum(picked[:1], axis=1, keepdims=True))
    for j in range(half):
        piece = jnp.where(core == 0, swapped_ref[j, :rows], returned_ref[j, :rows])
        for k in range(half):
            joined_ref[k, :, j * rows : (j + 1) * rows] = piece[:, k * rows : (k + 1) * rows]
    for k in range(half):
        straight = jnp.where(core == 0, returned_ref[k, :rows], swapped_ref[k, :rows])
        joined = joined_ref[k]
        sides = (jnp.where(core == 0, straight, joined), jnp.where(core == 0, joined, straight))
        for which, exchange in enumerate(sides):
            at = slice((2 * k + which) * width, (2 * k + which + 1) * width)
            coulomb = jnp.zeros(exchange.shape, jnp.float32)
            for aux in range(aux_count):
                coulomb += gammas[aux] * factor_ref[aux, :, at].astype(jnp.float32)
            fock = field_ref[:, at].astype(jnp.float32) + coulomb
            out_ref[:, at] = (fock - 0.25 * exchange.astype(jnp.float32)).astype(jnp.bfloat16)


def shards(factors, orbitals, field_term):
    aux_count, rows, half_n = factors.shape
    n = lax.axis_size(X)

    flat = factors.reshape(aux_count * rows, half_n)
    flat_other = other_core(flat)
    arrivals, places = piece_streams(orbitals)
    half, line = half_transform(flat, flat_other, arrivals, places)
    half = half.reshape(aux_count, rows, -1)

    pieces = []
    for aux in range(aux_count):
        for axis in (Y, X):
            pieces += row_pieces(half[aux], axis, aux % 2)
    depth = aux_count * half.shape[2]
    width = n // 2 * rows
    along, theirs = local_call(
        functools.partial(theirs_kernel, n, aux_count),
        (
            jax.ShapeDtypeStruct((2, n, rows, depth), jnp.bfloat16),
            jax.ShapeDtypeStruct((n * rows, width), jnp.bfloat16),
        ),
        pieces,
        2 * n * rows * width * depth,
    )
    arrived = other_core(theirs)
    mine, tile = local_call(
        functools.partial(mine_kernel, n, aux_count),
        (
            jax.ShapeDtypeStruct((n * rows, width), jnp.float32),
            jax.ShapeDtypeStruct((TILE, width), jnp.bfloat16),
        ),
        (along, line),
        2 * n * rows * width * depth,
    )
    packed = local_call(
        pack_kernel,
        jax.ShapeDtypeStruct((n, rows + TILE, width), jnp.bfloat16),
        (mine, arrived, tile),
        n * rows * width,
    )
    returned = lax.all_to_all(
        packed, (Y, X, "col"), 0, 0, axis_index_groups=core_groups(1), tiled=True
    )
    given = local_call(
        split_kernel,
        jax.ShapeDtypeStruct((n // 2, rows + TILE, width), jnp.bfloat16),
        (returned,),
        n * rows * width,
    )
    swapped = other_core(given)
    return local_call(
        functools.partial(final_kernel, aux_count),
        jax.ShapeDtypeStruct(field_term.shape, jnp.bfloat16),
        (returned, swapped, factors, field_term),
        8 * field_term.size,
        (pltpu.VMEM((n // 2, rows, width), jnp.bfloat16),),
    )


def solution(mesh):
    side = math.isqrt(mesh.shape["row"])
    finer = Mesh(
        mesh.devices.reshape(mesh.shape["grp"], side, side, mesh.shape["col"]),
        ("grp", Y, X, "col"),
    )
    return jax.shard_map(
        shards,
        mesh=finer,
        in_specs=(P(None, GRP_ROW, "col"), P(GRP_ROW, "col"), P(GRP_ROW, "col")),
        out_specs=P(GRP_ROW, "col"),
        check_vma=False,
    )
```
